32 devices in a mesh: sym: 4 (over y, x), row: 8 (over z, core).
Axes of the slice: x: 2, y: 2, z: 4, core: 2. Of those that a mesh axis runs over, the one named last changes fastest.
Arguments:
- inner_state: float32 [4, 6144, 128], P('sym', 'row'), may hold values from -6 to 6
- outer_state: float32 [4, 24, 128, 1024], P('sym', None, None, 'row'), may hold values from -6 to 6
- block_hamiltonian: bfloat16 [4, 6144, 6144], P('sym', 'row'), may hold values from -2 to 2, as said below
- dipole: bfloat16 [4, 6144, 6144], P('sym', 'row'), may hold values from -0.078125 to 0.078125
- field_strength: float32 [64], replicated, may hold values from -1.2 to 1.2
- dipole_links: int32 [3, 64], replicated, may hold values 0 or 1
- ghost_amplitude: float32 [4, 2, 6144], P('sym'), may hold values from -0.4 to 0.4
- surface_amplitude: float32 [4, 6144], P('sym'), may hold values from -3 to 3
- state_channel: int32 [4, 6144], P('sym'), may hold values from 0 to 23
- threshold: float32 [4, 24], P('sym'), may hold values from 0 to 1
Outputs:
- inner_next: float32 [4, 6144, 128], P('sym', 'row')
- outer_next: float32 [4, 24, 128, 1024], P('sym', None, None, 'row')
The draws below stay inside these ranges and needn't reach their ends.
Inputs may be any that keep to these rules, and one draw needn't show every extreme that they name: `block_hamiltonian`: each block is a symmetric matrix.
All inputs are finite; a program needn't handle non-finite values.
Results may differ from the reference program's by a relative error of at most 0.0085.
Values may be sent and summed in bfloat16 or wider, within the bound.
No kernel may reach another device: no remote copies, remote signals or barrier semaphores. Data moves between devices by JAX's collectives and lax.ppermute only.
A program may use at most 128 MiB of HBM per device.

```python
import math
import jax
import jax.numpy as jnp
from jax import lax

STATES = 6144
CHANNELS = 24
DELAYS = 64
TERMS = 4
BLOCKS = 4
RADIAL = 1024


def draw_block_hamiltonian(key, part):
    keys = jax.random.split(key, BLOCKS)

    def make_block(one_key):
        random_part = jax.random.normal(one_key, (STATES, STATES), jnp.float32)
        symmetric = (random_part + random_part.T) / math.sqrt(2.0 * STATES)
        energies = jax.random.uniform(jax.random.fold_in(one_key, 7), (STATES,), jnp.float32, -1.0, 1.0)
        return (symmetric + jnp.diag(energies)).astype(jnp.bfloat16)
    return lax.map(make_block, keys)


def set_ends(values, own_key, smallest, high):
    shape = values.shape
    place = [jax.random.randint(jax.random.fold_in(own_key, axis), (), 0, shape[axis]) for axis in range(len(shape))]
    values = values.at[tuple(place)].set(smallest)
    longest = shape.index(max(shape))
    place[longest] = (place[longest] + 1) % shape[longest]
    return values.at[tuple(place)].set(high)


def steps_of(rng, shape, shards, least, largest):
    factor_of = 1.0
    for position, blocks in shards:
        draws = jax.random.uniform(jax.random.fold_in(jax.random.fold_in(rng, 6), position), (blocks,), jnp.float32, least / len(shards), largest / len(shards))
        factor_of = factor_of * jnp.repeat(jnp.exp(draws), shape[position] // blocks).reshape((-1,) + (1,) * (len(shape) - 1 - position))
    return factor_of


def bell_draw(own_key, shape, deviation, limit, cuts=(), kind=jnp.bfloat16):
    values = jax.random.normal(own_key, shape, jnp.float32) * deviation
    if len(cuts) > 0:
        values = steps_of(own_key, shape, cuts, -0.22, 0.18) * values
    return jnp.clip(values, min=-limit, max=limit).astype(kind)


def setup_inputs(seed: int = 0) -> dict:
    arg_keys = jax.random.split(jax.random.key(seed), 11)
    return {
        "inner_state": bell_draw(arg_keys[0], (BLOCKS, STATES, 2 * DELAYS), 1.0, 6.0, ((0, 4), (1, 8)), jnp.float32),
        "outer_state": bell_draw(arg_keys[1], (BLOCKS, CHANNELS, 2 * DELAYS, RADIAL), 1.0, 6.0, ((0, 4), (3, 8)), jnp.float32),
        "block_hamiltonian": draw_block_hamiltonian(jax.random.fold_in(arg_keys[10], 71), 0),
        "dipole": bell_draw(arg_keys[3], (BLOCKS, STATES, STATES), STATES ** -0.5, 0.078125, ((0, 4), (1, 8))),
        "field_strength": bell_draw(arg_keys[4], (DELAYS,), 0.3, 1.2, (), jnp.float32),
        "dipole_links": set_ends((jax.random.randint(arg_keys[5], (BLOCKS - 1, DELAYS), 0, 2) < 1).astype(jnp.int32), jax.random.fold_in(arg_keys[5], 1), 0, 1),
        "ghost_amplitude": bell_draw(arg_keys[6], (BLOCKS, 2, STATES), 0.0625, 0.4, ((0, 4),), jnp.float32),
        "surface_amplitude": bell_draw(arg_keys[7], (BLOCKS, STATES), 0.5, 3.0, ((0, 4),), jnp.float32),
        "state_channel": set_ends(jax.random.randint(arg_keys[8], (BLOCKS, STATES), 0, CHANNELS), jax.random.fold_in(arg_keys[8], 1), 0, CHANNELS - 1).astype(jnp.int32),
        "threshold": jnp.clip(1.0 * jax.random.uniform(arg_keys[9], (BLOCKS, CHANNELS), jnp.float32) ** steps_of(arg_keys[9], (BLOCKS, CHANNELS), ((0, 4),), -0.2, 0.2), 0.0, 1.0),
    }


time_step = 2.0
spacing = 1.5
radius_start = 20.0
charge = 1.0


def plain_products(matrices, vectors):
    def single(operands):
        return jnp.dot(operands[0], operands[1], preferred_element_type=jnp.float32)
    return lax.map(single, (matrices, vectors))


def transposed_products(matrices, vectors):
    def single(operands):
        return jnp.dot(operands[0].T, operands[1], preferred_element_type=jnp.float32)
    return lax.map(single, (matrices, vectors))


def rotate(values, factor, axis):
    real_part, imag_part = jnp.split(values, 2, axis=axis)
    return jnp.concatenate([factor * imag_part, -factor * real_part], axis=axis)


def reference(inner_state, outer_state, block_hamiltonian, dipole, field_strength, dipole_links, ghost_amplitude, surface_amplitude, state_channel, threshold):
    channel_hot = (state_channel[:, :, None] == jnp.arange(CHANNELS, dtype=jnp.int32)[None, None, :]).astype(jnp.float32)
    radius = radius_start + spacing * jnp.arange(RADIAL).astype(jnp.float32)
    potential = threshold[:, :, None] - charge / radius[None, None, :]
    column_field = jnp.concatenate([field_strength, field_strength])
    links_float = dipole_links.astype(jnp.float32)
    coupled = jnp.concatenate([links_float, jnp.zeros((1, links_float.shape[1]), jnp.float32)], axis=0)
    coupled = jnp.concatenate([coupled, coupled], axis=1)
    weighted = ghost_amplitude[:, :, :, None] * channel_hot[:, None, :, :]
    inner_vec = inner_state
    outer_vec = outer_state
    inner_total = inner_state
    outer_total = outer_state
    for order in range(1, TERMS + 1):
        rounded = inner_vec.astype(jnp.bfloat16)
        ghost = jnp.einsum('ljpc,lpq->ljcq', weighted, rounded.astype(jnp.float32), precision=lax.Precision.HIGHEST)
        slope = (outer_vec[:, :, :, 1] - ghost[:, 0]) / (2.0 * spacing)
        padded = jnp.concatenate([ghost[:, 1][..., None], ghost[:, 0][..., None], outer_vec,
                                  jnp.zeros(outer_vec.shape[:3] + (2,), jnp.float32)], axis=-1)
        laplace = (-padded[..., :-4] + 16.0 * padded[..., 1:-3] - 30.0 * padded[..., 2:-2]
                   + 16.0 * padded[..., 3:-1] - padded[..., 4:]) / (12.0 * spacing * spacing)
        outer_image = -0.5 * laplace + potential[:, :, None, :] * outer_vec
        hamiltonian_part = plain_products(block_hamiltonian, rounded)
        upper_vectors = jnp.concatenate([rounded[1:], jnp.zeros_like(rounded[:1])], axis=0)
        upper_part = plain_products(dipole, upper_vectors)
        lifted = transposed_products(dipole, rounded) * coupled[:, None, :]
        lower_part = jnp.concatenate([jnp.zeros_like(lifted[:1]), lifted[:-1]], axis=0)
        source = jnp.einsum('lpc,lcq->lpq', channel_hot, slope, precision=lax.Precision.HIGHEST)
        inner_image = (hamiltonian_part
                       + column_field[None, None, :] * (coupled[:, None, :] * upper_part + lower_part)
                       + 0.5 * surface_amplitude[:, :, None] * source)
        factor = time_step / order
        inner_vec = rotate(inner_image, factor, 2)
        outer_vec = rotate(outer_image, factor, 2)
        inner_total = inner_total + inner_vec
        outer_total = outer_total + outer_vec
    return inner_total, outer_total
```

```python
import jax
import jax.numpy as jnp
from jax import lax
from jax.experimental import pallas as pl
from jax.experimental.pallas import tpu as pltpu
from jax.sharding import PartitionSpec as P


TERMS = 4
CORES = 2

time_step = 2.0
spacing = 1.5
radius_start = 20.0
charge = 1.0


BF16 = jnp.bfloat16
F32 = jnp.float32


def dot(a, b):
    return jnp.dot(a, b, preferred_element_type=F32)


def partner(i, by):
    return ((i // CORES) ^ by) * CORES + i % CORES


def chip_swap(x, by):
    total = lax.axis_size("row")
    return lax.ppermute(x, "row", [(i, partner(i, by)) for i in range(total)])


def core_swap(x):
    total = lax.axis_size("row")
    return lax.ppermute(x, "row", [(i, i ^ 1) for i in range(total)])


def to_block_below(x):
    count = lax.axis_size("sym")
    return lax.ppermute(x, "sym", [(i, i - 1) for i in range(1, count)])


def to_block_above(x):
    count = lax.axis_size("sym")
    return lax.ppermute(x, "sym", [(i, i + 1) for i in range(count - 1)])


def from_first_row(x):
    total = lax.axis_size("row")
    x = jnp.where(lax.axis_index("row") == 0, x, jnp.zeros_like(x))
    reach = 1
    while reach < total:
        pairs = [(i, i + reach) for i in range(reach) if i + reach < total]
        x = x + lax.ppermute(x, "row", pairs)
        reach *= 2
    return x


VMEM = pl.BlockSpec(memory_space=pltpu.VMEM)
SMEM = pl.BlockSpec(memory_space=pltpu.SMEM)


def local_call(kernel, out_shape, in_specs, operands, flops=0, scratch=()):
    return pl.pallas_call(
        kernel,
        in_specs=in_specs,
        out_specs=[VMEM] * len(out_shape),
        out_shape=out_shape,
        scratch_shapes=list(scratch),
        compiler_params=pltpu.CompilerParams(vmem_limit_bytes=7 * 2**20),
        cost_estimate=pl.CostEstimate(flops=flops, bytes_accessed=0, transcendentals=0),
    )(*operands)


def columns_of(index_ref, j, rows):
    return pl.ds(pl.multiple_of(index_ref[j] * rows, 128), rows)


def give_kernel(index_ref, d_ref, u_ref, out_ref, ut_ref):
    rows = u_ref.shape[0]
    ut_ref[...] = u_ref[...].astype(F32).T.astype(BF16)
    for k in range(out_ref.shape[0]):
        part = dot(ut_ref[...], d_ref[:, columns_of(index_ref, k, rows)])
        out_ref[k] = part.T.astype(BF16)


def lift_give(index, dipole_rows, u):
    rows, columns = u.shape
    chips = index.shape[0]
    return local_call(
        give_kernel,
        [
            jax.ShapeDtypeStruct((chips, rows, columns), BF16),
            jax.ShapeDtypeStruct((columns, rows), BF16),
        ],
        [SMEM, VMEM, VMEM],
        [index, dipole_rows, u],
        flops=2 * rows * rows * chips * columns,
    )


def keep_kernel(index_ref, d_ref, ut_ref, carry_ref, *rest):
    *outs, token = rest
    rows = ut_ref.shape[1]
    for k, out in enumerate(outs):
        part = dot(ut_ref[...], d_ref[:, columns_of(index_ref, k, rows)])
        out[...] = (part.T + carry_ref[k].astype(F32)).astype(BF16)
    token[...] = jnp.zeros_like(token)


def lift_keep(index, dipole_rows, ut, carry):
    columns, rows = ut.shape
    chips = index.shape[0]
    *lifted, token = local_call(
        keep_kernel,
        [jax.ShapeDtypeStruct((rows, columns), BF16)] * chips
        + [jax.ShapeDtypeStruct((8, 128), F32)],
        [SMEM, VMEM, VMEM, VMEM],
        [index, dipole_rows, ut, carry],
        flops=2 * rows * rows * chips * columns,
    )
    return lifted, token


def stack_kernel(token, *refs):
    *pieces_in, out = refs
    for k, ref in enumerate(pieces_in):
        out[k] = ref[...]


def stack(arrays, token):
    rows, columns = arrays[0].shape
    return local_call(
        stack_kernel,
        [jax.ShapeDtypeStruct((len(arrays), rows, columns), BF16)],
        [VMEM] * (1 + len(arrays)),
        [token, *arrays],
    )[0]


def assemble(index_ref, whole, refs):
    rows = refs[0].shape[0]
    j = 0
    for ref in refs:
        views = [ref] if len(ref.shape) == 2 else [ref.at[k] for k in range(ref.shape[0])]
        for view in views:
            whole[pl.ds(pl.multiple_of(index_ref[j] * rows, 128), rows), :] = view[...]
            j += 1


def row_dots(out, matrix, whole, finish):
    half = out.shape[0] // 2

    def step(i, carry):
        where = pl.ds(pl.multiple_of(i * half, 8), half)
        finish(where, dot(matrix[where, :], whole[...]))
        return carry

    lax.fori_loop(0, 2, step, 0)


def own_kernel(index_ref, h_ref, g_ref, *rest):
    *refs, y_ref, ghost_ref, whole = rest
    assemble(index_ref, whole, refs)

    def finish(where, product):
        y_ref[where, :] = product

    row_dots(y_ref, h_ref, whole, finish)
    ghosts = ghost_ref.shape[0]
    ghost = dot(g_ref[...], whole[...])
    ghost_ref[...] = ghost[:ghosts] + ghost[ghosts:]


def own_product(index, held, ghosts, refs):
    rows, columns = refs[0].shape
    states = held.shape[1]
    return local_call(
        own_kernel,
        [
            jax.ShapeDtypeStruct((rows, columns), F32),
            jax.ShapeDtypeStruct((ghosts.shape[0] // 2, columns), F32),
        ],
        [SMEM] + [VMEM] * (2 + len(refs)),
        [index, held, ghosts, *refs],
        flops=2 * held.shape[0] * states * columns,
        scratch=[pltpu.VMEM((states, columns), BF16)],
    )


def near_kernel(
    ghost_ref, near_ref, near_total_ref, potential_ref, sign_ref,
    slope_ref, near_out, near_total_out,
):
    channels = near_ref.shape[1]
    ghost_0, ghost_1 = ghost_ref[:channels], ghost_ref[channels:]
    slope = (near_ref[1] - ghost_0) * (1.0 / (2.0 * spacing))
    slope_ref[...] = jnp.zeros_like(slope_ref)
    for i in range(3):
        top = slope.astype(BF16)
        slope = slope - top.astype(F32)
        slope_ref[i * channels : (i + 1) * channels, :] = top
    count = near_ref.shape[0]
    points = [ghost_1, ghost_0] + [near_ref[i] for i in range(count)]
    half = ghost_0.shape[1] // 2
    for i in range(count - 2):
        laplace = (
            -points[i] + 16.0 * points[i + 1] - 30.0 * points[i + 2]
            + 16.0 * points[i + 3] - points[i + 4]
        ) * (1.0 / (12.0 * spacing * spacing))
        image = -0.5 * laplace + potential_ref[i] * points[i + 2]
        turned = pltpu.roll(image, half, 1) * sign_ref[0:1]
        near_out[i] = turned
        if i < near_total_ref.shape[0]:
            near_total_out[i] = near_total_ref[i] + turned


def near_step(ghost, near, near_total, potential, sign, depth):
    columns = near.shape[2]
    return local_call(
        near_kernel,
        [
            jax.ShapeDtypeStruct((depth, columns), BF16),
            jax.ShapeDtypeStruct((near.shape[0] - 2, *near.shape[1:]), F32),
            jax.ShapeDtypeStruct(near_total.shape, F32),
        ],
        [VMEM] * 5,
        [ghost, near, near_total, potential, sign],
    )


def settle_kernel(*refs):
    *terms, out = refs
    total = terms[0][...].astype(F32)
    for term in terms[1:]:
        total = total + term[...].astype(F32)
    out[...] = total.astype(BF16)


def settle(terms):
    return local_call(
        settle_kernel,
        [jax.ShapeDtypeStruct(terms[0].shape, BF16)],
        [VMEM] * len(terms),
        terms,
    )[0]


def upper_kernel(
    index_ref, d_ref, y_ref, hot_ref, slope_ref, surface_ref, vectors_ref, *rest
):
    *refs, out, whole = rest
    assemble(index_ref, whole, refs)

    def finish(where, product):
        source = dot(hot_ref[where, :], slope_ref[...])
        out[where, :] = (
            y_ref[where, :]
            + vectors_ref[0:1] * product
            + surface_ref[where, :] * source
        )

    row_dots(out, d_ref, whole, finish)


def upper_product(index, held, y, hot, slope, surface, vectors, refs):
    rows, columns = refs[0].shape
    states = held.shape[1]
    operands = [index, held, y, hot, slope, surface, vectors, *refs]
    return local_call(
        upper_kernel,
        [jax.ShapeDtypeStruct((rows, columns), F32)],
        [SMEM] + [VMEM] * (len(operands) - 1),
        operands,
        flops=2 * rows * states * columns,
        scratch=[pltpu.VMEM((states, columns), BF16)],
    )[0]


def close_kernel(image_ref, lower_ref, vectors_ref, total_ref, *outs):
    image = image_ref[...] + vectors_ref[1:2] * lower_ref[...].astype(F32)
    vec = pltpu.roll(image, image.shape[1] // 2, 1) * vectors_ref[2:3]
    outs[0][...] = total_ref[...] + vec
    if len(outs) > 1:
        outs[1][...] = vec.astype(BF16)


def close_order(image, lower, vectors, total, last):
    out_shape = [jax.ShapeDtypeStruct(image.shape, F32)]
    if not last:
        out_shape.append(jax.ShapeDtypeStruct(image.shape, BF16))
    return local_call(
        close_kernel, out_shape, [VMEM] * 4, [image, lower, vectors, total]
    )


def pieces(x, count):
    found = []
    for _ in range(count):
        top = lax.reduce_precision(x, 8, 7)
        found.append(top.astype(BF16))
        x = x - top
    return found


def rotate(values, factor):
    real_part, imag_part = jnp.split(values, 2, axis=-1)
    return jnp.concatenate([factor * imag_part, -factor * real_part], axis=-1)


def outer_step(w, potential):
    laplace = (-w[:-4] + 16.0 * w[1:-3] - 30.0 * w[2:-2] + 16.0 * w[3:-1] - w[4:]) / (
        12.0 * spacing * spacing
    )
    return -0.5 * laplace + potential * w[2:-2]


def per_device(
    inner_state,
    outer_state,
    block_hamiltonian,
    dipole,
    field_strength,
    dipole_links,
    ghost_amplitude,
    surface_amplitude,
    state_channel,
    threshold,
):
    hamiltonian_rows = block_hamiltonian[0]
    dipole_rows = dipole[0]
    rows, states = hamiltonian_rows.shape
    columns = inner_state.shape[2]
    channels = threshold.shape[1]
    radial_here = outer_state.shape[3]
    block_index = lax.axis_index("sym")
    row_index = lax.axis_index("row")
    row_count = lax.axis_size("row")
    chips = row_count // CORES
    chip, core = row_index // CORES, row_index % CORES
    margin = 2 * TERMS

    steps = jnp.arange(chips, dtype=jnp.int32)
    away = chip ^ steps
    give_index = away * CORES + 1 - core
    keep_index = away * CORES + core
    gather_index = jnp.concatenate([keep_index, give_index])

    link_float = dipole_links.astype(F32)
    link_zero = jnp.zeros((1, link_float.shape[1]), F32)
    link_table = jnp.concatenate([link_zero, link_float, link_zero], axis=0)
    link_pair = lax.dynamic_slice_in_dim(link_table, block_index, 2, 0)
    link_pair = jnp.concatenate([link_pair, link_pair], axis=1)
    column_field = jnp.concatenate([field_strength, field_strength])
    upper_factor = column_field * link_pair[1]
    lower_factor = column_field * link_pair[0]
    half_sign = jnp.where(jnp.arange(columns) < columns // 2, 1.0, -1.0).astype(F32)

    channel_ids = jnp.arange(channels, dtype=jnp.int32)
    all_hot = (channel_ids[:, None] == state_channel[0][None, :]).astype(F32)
    weighted = (ghost_amplitude[0][:, None, :] * all_hot[None]).reshape(2 * channels, states)
    ghost_matrix = jnp.concatenate(pieces(weighted, 2), axis=0)
    own_channel = lax.dynamic_slice_in_dim(state_channel[0], row_index * rows, rows, 0)
    own_surface = lax.dynamic_slice_in_dim(surface_amplitude[0], row_index * rows, rows, 0)
    depth = 128 * ((3 * channels + 127) // 128)
    slot = jnp.arange(depth, dtype=jnp.int32)
    own_hot = (
        (own_channel[:, None] == (slot % channels)[None, :]) & (slot < 3 * channels)[None, :]
    ).astype(BF16)
    half_surface = 0.5 * own_surface[:, None]

    outer0 = jnp.transpose(outer_state[0], (2, 0, 1))
    forward = [(i, i + 1) for i in range(row_count - 1)]
    backward = [(i + 1, i) for i in range(row_count - 1)]
    low = lax.ppermute(outer0[radial_here - margin :], "row", forward)
    high = lax.ppermute(outer0[:margin], "row", backward)
    near = from_first_row(outer0[: 2 * margin])

    def potential_at(points):
        radius = radius_start + spacing * points.astype(F32)
        return (threshold[0][None, :] - charge / radius[:, None])[:, :, None]

    near_potential = jnp.broadcast_to(
        potential_at(jnp.arange(2 * margin, dtype=jnp.int32)), near.shape
    )
    near_total = near[:margin]

    rounded = inner_state[0].astype(BF16)
    inner_total = inner_state[0]
    for order in range(1, TERMS + 1):
        factor = time_step / order
        sign = (factor * half_sign)[None]
        above = to_block_below(rounded)
        around = []
        for k in range(1, chips):
            around.append(chip_swap(rounded, k))
        rounded_other = core_swap(rounded)
        given, turned = lift_give(give_index, dipole_rows, rounded)
        carried = core_swap(given)
        lifted, token = lift_keep(keep_index, dipole_rows, turned, carried)
        landed = [lifted[0]]
        for k in reversed(range(1, chips)):
            landed.append(chip_swap(lifted[k], k))
        above_next = to_block_below(around[0])
        next_other = core_swap(around[0])
        own = stack(around[1:], token)
        above_own = to_block_below(own)
        own_other = core_swap(own)
        part, ghost = own_product(
            gather_index, hamiltonian_rows, ghost_matrix,
            [rounded, around[0], own, rounded_other, next_other, own_other],
        )
        slope, near, near_total = near_step(
            ghost, near, near_total, near_potential, sign, depth
        )
        vectors = jnp.stack([upper_factor, lower_factor, factor * half_sign])
        above_other = core_swap(above)
        next_above_other = core_swap(above_next)
        above_own_other = core_swap(above_own)
        settled = settle(landed)
        lower = to_block_above(settled)
        image = upper_product(
            gather_index, dipole_rows, part, own_hot, slope, half_surface, vectors,
            [above, above_next, above_own, above_other, next_above_other,
             above_own_other],
        )
        closed = close_order(image, lower, vectors, inner_total, order == TERMS)
        inner_total = closed[0]
        rounded = closed[-1]

    points = row_index * radial_here - margin + jnp.arange(
        radial_here + 2 * margin, dtype=jnp.int32
    )
    inside = (points < row_count * radial_here)[:, None, None]
    slab_potential = potential_at(points)
    w = jnp.concatenate([low, outer0, high], axis=0)
    outer_total = outer0
    for order in range(1, TERMS + 1):
        trim = slice(2 * order, points.shape[0] - 2 * order)
        w = rotate(outer_step(w, slab_potential[trim]), time_step / order)
        w = jnp.where(inside[trim], w, 0.0)
        extra = margin - 2 * order
        outer_total = outer_total + w[extra : extra + radial_here]
    first = jnp.where(row_index == 0, near_total, outer_total[:margin])
    outer_total = jnp.concatenate([first, outer_total[margin:]], axis=0)
    outer_total = jnp.transpose(outer_total, (1, 2, 0))
    return inner_total[None], outer_total[None]


def solution(mesh):
    return jax.shard_map(
        per_device,
        mesh=mesh,
        in_specs=(
            P("sym", "row", None),
            P("sym", None, None, "row"),
            P("sym", "row", None),
            P("sym", "row", None),
            P(),
            P(),
            P("sym", None, None),
            P("sym", None),
            P("sym", None),
            P("sym", None),
        ),
        out_specs=(P("sym", "row", None), P("sym", None, None, "row")),
        check_vma=False,
    )
```

```python
import jax
import jax.numpy as jnp
from jax import lax
from jax.experimental import pallas as pl
from jax.experimental.pallas import tpu as pltpu
from jax.sharding import PartitionSpec as P


TERMS = 4
CORES = 2

time_step = 2.0
spacing = 1.5
radius_start = 20.0
charge = 1.0


BF16 = jnp.bfloat16
F32 = jnp.float32


def dot(a, b):
    return jnp.dot(a, b, preferred_element_type=F32)


def partner(i, by):
    return ((i // CORES) ^ by) * CORES + i % CORES


def chip_swap(x, by):
    total = lax.axis_size("row")
    return lax.ppermute(x, "row", [(i, partner(i, by)) for i in range(total)])


def core_swap(x):
    total = lax.axis_size("row")
    return lax.ppermute(x, "row", [(i, i ^ 1) for i in range(total)])


def to_block_below(x):
    count = lax.axis_size("sym")
    return lax.ppermute(x, "sym", [(i, i - 1) for i in range(1, count)])


def to_block_above(x):
    count = lax.axis_size("sym")
    return lax.ppermute(x, "sym", [(i, i + 1) for i in range(count - 1)])


def from_first_row(x):
    total = lax.axis_size("row")
    x = jnp.where(lax.axis_index("row") == 0, x, jnp.zeros_like(x))
    reach = 1
    while reach < total:
        pairs = [(i, i + reach) for i in range(reach) if i + reach < total]
        x = x + lax.ppermute(x, "row", pairs)
        reach *= 2
    return x


VMEM = pl.BlockSpec(memory_space=pltpu.VMEM)
SMEM = pl.BlockSpec(memory_space=pltpu.SMEM)
HBM = pl.BlockSpec(memory_space=pltpu.HBM)
STREAM_GRANT = 47
ROW_PARTS = 4
SUB_COPIES = 6
BLOCK_COPIES = 4


def local_call(kernel, out_shape, in_specs, operands, flops=0, scratch=(), grant=7):
    return pl.pallas_call(
        kernel,
        in_specs=in_specs,
        out_specs=[VMEM] * len(out_shape),
        out_shape=out_shape,
        scratch_shapes=list(scratch),
        compiler_params=pltpu.CompilerParams(vmem_limit_bytes=grant * 2**20),
        cost_estimate=pl.CostEstimate(flops=flops, bytes_accessed=0, transcendentals=0),
    )(*operands)


def columns_of(index_ref, j, rows):
    return pl.ds(pl.multiple_of(index_ref[j] * rows, 128), rows)


def column_copies(index_ref, d_ref, held, sems, k):
    rows = held.shape[1]
    part = rows // BLOCK_COPIES
    return [
        pltpu.make_async_copy(
            d_ref.at[pl.ds(i * part, part), columns_of(index_ref, k, rows)],
            held.at[k, pl.ds(i * part, part)],
            sems.at[k, i],
        )
        for i in range(BLOCK_COPIES)
    ]


def each(count, act):
    def step(k, carry):
        act(k)
        return carry

    lax.fori_loop(0, count, step, 0)


def start_all(copies):
    for copy in copies:
        copy.start()


def wait_all(copies):
    for copy in copies:
        copy.wait()


def give_kernel(index_ref, d_ref, u_ref, out_ref, ut_ref, held, sems):
    chips = held.shape[0]
    each(chips, lambda k: start_all(column_copies(index_ref, d_ref, held, sems, k)))
    ut_ref[...] = u_ref[...].astype(F32).T.astype(BF16)

    def block(k):
        wait_all(column_copies(index_ref, d_ref, held, sems, k))
        out_ref[k] = dot(ut_ref[...], held[k]).T.astype(BF16)

    each(chips, block)


def column_scratch(chips, rows):
    return [pltpu.VMEM((chips, rows, rows), BF16), pltpu.SemaphoreType.DMA((chips, BLOCK_COPIES))]


def lift_give(index, dipole_rows, u):
    rows, columns = u.shape
    chips = index.shape[0]
    return local_call(
        give_kernel,
        [
            jax.ShapeDtypeStruct((chips, rows, columns), BF16),
            jax.ShapeDtypeStruct((columns, rows), BF16),
        ],
        [SMEM, HBM, VMEM],
        [index, dipole_rows, u],
        flops=2 * rows * rows * chips * columns,
        scratch=column_scratch(chips, rows),
        grant=STREAM_GRANT,
    )


def keep_kernel(index_ref, d_ref, ut_ref, carry_ref, *rest):
    *outs, token, held, sems = rest
    chips = held.shape[0]
    each(chips, lambda k: start_all(column_copies(index_ref, d_ref, held, sems, k)))
    for k, out in enumerate(outs):
        wait_all(column_copies(index_ref, d_ref, held, sems, k))
        part = dot(ut_ref[...], held[k]).T
        out[...] = (part + carry_ref[k].astype(F32)).astype(BF16)
    token[...] = jnp.zeros_like(token)


def lift_keep(index, dipole_rows, ut, carry):
    columns, rows = ut.shape
    chips = index.shape[0]
    *lifted, token = local_call(
        keep_kernel,
        [jax.ShapeDtypeStruct((rows, columns), BF16)] * chips
        + [jax.ShapeDtypeStruct((8, 128), F32)],
        [SMEM, HBM, VMEM, VMEM],
        [index, dipole_rows, ut, carry],
        flops=2 * rows * rows * chips * columns,
        scratch=column_scratch(chips, rows),
        grant=STREAM_GRANT,
    )
    return lifted, token


def stack_kernel(token, *refs):
    *pieces_in, out = refs
    for k, ref in enumerate(pieces_in):
        out[k] = ref[...]


def stack(arrays, token):
    rows, columns = arrays[0].shape
    return local_call(
        stack_kernel,
        [jax.ShapeDtypeStruct((len(arrays), rows, columns), BF16)],
        [VMEM] * (1 + len(arrays)),
        [token, *arrays],
    )[0]


def assemble(index_ref, whole, refs):
    rows = refs[0].shape[0]
    j = 0
    for ref in refs:
        views = [ref] if len(ref.shape) == 2 else [ref.at[k] for k in range(ref.shape[0])]
        for view in views:
            whole[pl.ds(pl.multiple_of(index_ref[j] * rows, 128), rows), :] = view[...]
            j += 1


def row_copies(matrix, held, sems, i):
    part = held.shape[0] // ROW_PARTS
    sub = part // SUB_COPIES
    places = [pl.ds(pl.multiple_of(i * part + n * sub, sub), sub) for n in range(SUB_COPIES)]
    return [
        pltpu.make_async_copy(matrix.at[at], held.at[at], sems.at[i, n])
        for n, at in enumerate(places)
    ]


def row_dots(matrix, held, sems, whole, prepare, finish):
    part = held.shape[0] // ROW_PARTS
    each(ROW_PARTS, lambda i: start_all(row_copies(matrix, held, sems, i)))
    prepare()

    def block(i):
        wait_all(row_copies(matrix, held, sems, i))
        where = pl.ds(pl.multiple_of(i * part, part), part)
        finish(where, dot(held[where, :], whole[...]))

    each(ROW_PARTS, block)


def row_scratch(held, columns):
    return [
        pltpu.VMEM((held.shape[1], columns), BF16),
        pltpu.VMEM(held.shape, BF16),
        pltpu.SemaphoreType.DMA((ROW_PARTS, SUB_COPIES)),
    ]


def own_kernel(index_ref, h_ref, g_ref, *rest):
    *refs, y_ref, ghost_ref, whole, held, sems = rest

    def prepare():
        assemble(index_ref, whole, refs)
        ghosts = ghost_ref.shape[0]
        ghost = dot(g_ref[...], whole[...])
        ghost_ref[...] = ghost[:ghosts] + ghost[ghosts:]

    def finish(where, product):
        y_ref[where, :] = product

    row_dots(h_ref, held, sems, whole, prepare, finish)


def own_product(index, held, ghosts, refs):
    rows, columns = refs[0].shape
    states = held.shape[1]
    return local_call(
        own_kernel,
        [
            jax.ShapeDtypeStruct((rows, columns), F32),
            jax.ShapeDtypeStruct((ghosts.shape[0] // 2, columns), F32),
        ],
        [SMEM, HBM] + [VMEM] * (1 + len(refs)),
        [index, held, ghosts, *refs],
        flops=2 * held.shape[0] * states * columns,
        scratch=row_scratch(held, columns),
        grant=STREAM_GRANT,
    )


def near_kernel(
    ghost_ref, near_ref, near_total_ref, potential_ref, sign_ref,
    slope_ref, near_out, near_total_out,
):
    channels = near_ref.shape[1]
    ghost_0, ghost_1 = ghost_ref[:channels], ghost_ref[channels:]
    slope = (near_ref[1] - ghost_0) * (1.0 / (2.0 * spacing))
    slope_ref[...] = jnp.zeros_like(slope_ref)
    for i in range(3):
        top = slope.astype(BF16)
        slope = slope - top.astype(F32)
        slope_ref[i * channels : (i + 1) * channels, :] = top
    count = near_ref.shape[0]
    points = [ghost_1, ghost_0] + [near_ref[i] for i in range(count)]
    half = ghost_0.shape[1] // 2
    for i in range(count - 2):
        laplace = (
            -points[i] + 16.0 * points[i + 1] - 30.0 * points[i + 2]
            + 16.0 * points[i + 3] - points[i + 4]
        ) * (1.0 / (12.0 * spacing * spacing))
        image = -0.5 * laplace + potential_ref[i] * points[i + 2]
        turned = pltpu.roll(image, half, 1) * sign_ref[0:1]
        near_out[i] = turned
        if i < near_total_ref.shape[0]:
            near_total_out[i] = near_total_ref[i] + turned


def near_step(ghost, near, near_total, potential, sign, depth):
    columns = near.shape[2]
    return local_call(
        near_kernel,
        [
            jax.ShapeDtypeStruct((depth, columns), BF16),
            jax.ShapeDtypeStruct((near.shape[0] - 2, *near.shape[1:]), F32),
            jax.ShapeDtypeStruct(near_total.shape, F32),
        ],
        [VMEM] * 5,
        [ghost, near, near_total, potential, sign],
    )


def settle_kernel(*refs):
    *terms, out = refs
    total = terms[0][...].astype(F32)
    for term in terms[1:]:
        total = total + term[...].astype(F32)
    out[...] = total.astype(BF16)


def settle(terms):
    return local_call(
        settle_kernel,
        [jax.ShapeDtypeStruct(terms[0].shape, BF16)],
        [VMEM] * len(terms),
        terms,
    )[0]


def upper_kernel(
    index_ref, d_ref, y_ref, hot_ref, slope_ref, surface_ref, vectors_ref, *rest
):
    *refs, out, whole, held, sems = rest

    def finish(where, product):
        source = dot(hot_ref[where, :], slope_ref[...])
        out[where, :] = (
            y_ref[where, :]
            + vectors_ref[0:1] * product
            + surface_ref[where, :] * source
        )

    row_dots(
        d_ref, held, sems, whole, lambda: assemble(index_ref, whole, refs), finish
    )


def upper_product(index, held, y, hot, slope, surface, vectors, refs):
    rows, columns = refs[0].shape
    states = held.shape[1]
    operands = [index, held, y, hot, slope, surface, vectors, *refs]
    return local_call(
        upper_kernel,
        [jax.ShapeDtypeStruct((rows, columns), F32)],
        [SMEM, HBM] + [VMEM] * (len(operands) - 2),
        operands,
        flops=2 * rows * states * columns,
        scratch=row_scratch(held, columns),
        grant=STREAM_GRANT,
    )[0]


def close_kernel(image_ref, lower_ref, vectors_ref, total_ref, *outs):
    image = image_ref[...] + vectors_ref[1:2] * lower_ref[...].astype(F32)
    vec = pltpu.roll(image, image.shape[1] // 2, 1) * vectors_ref[2:3]
    outs[0][...] = total_ref[...] + vec
    if len(outs) > 1:
        outs[1][...] = vec.astype(BF16)


def close_order(image, lower, vectors, total, last):
    out_shape = [jax.ShapeDtypeStruct(image.shape, F32)]
    if not last:
        out_shape.append(jax.ShapeDtypeStruct(image.shape, BF16))
    return local_call(
        close_kernel, out_shape, [VMEM] * 4, [image, lower, vectors, total]
    )


def pieces(x, count):
    found = []
    for _ in range(count):
        top = lax.reduce_precision(x, 8, 7)
        found.append(top.astype(BF16))
        x = x - top
    return found


def rotate(values, factor):
    real_part, imag_part = jnp.split(values, 2, axis=-1)
    return jnp.concatenate([factor * imag_part, -factor * real_part], axis=-1)


def outer_step(w, potential):
    laplace = (-w[:-4] + 16.0 * w[1:-3] - 30.0 * w[2:-2] + 16.0 * w[3:-1] - w[4:]) / (
        12.0 * spacing * spacing
    )
    return -0.5 * laplace + potential * w[2:-2]


def per_device(
    inner_state,
    outer_state,
    block_hamiltonian,
    dipole,
    field_strength,
    dipole_links,
    ghost_amplitude,
    surface_amplitude,
    state_channel,
    threshold,
):
    hamiltonian_rows = block_hamiltonian[0]
    dipole_rows = dipole[0]
    rows, states = hamiltonian_rows.shape
    columns = inner_state.shape[2]
    channels = threshold.shape[1]
    radial_here = outer_state.shape[3]
    block_index = lax.axis_index("sym")
    row_index = lax.axis_index("row")
    row_count = lax.axis_size("row")
    chips = row_count // CORES
    chip, core = row_index // CORES, row_index % CORES
    margin = 2 * TERMS

    steps = jnp.arange(chips, dtype=jnp.int32)
    away = chip ^ steps
    give_index = away * CORES + 1 - core
    keep_index = away * CORES + core
    gather_index = jnp.concatenate([keep_index, give_index])

    link_float = dipole_links.astype(F32)
    link_zero = jnp.zeros((1, link_float.shape[1]), F32)
    link_table = jnp.concatenate([link_zero, link_float, link_zero], axis=0)
    link_pair = lax.dynamic_slice_in_dim(link_table, block_index, 2, 0)
    link_pair = jnp.concatenate([link_pair, link_pair], axis=1)
    column_field = jnp.concatenate([field_strength, field_strength])
    upper_factor = column_field * link_pair[1]
    lower_factor = column_field * link_pair[0]
    half_sign = jnp.where(jnp.arange(columns) < columns // 2, 1.0, -1.0).astype(F32)

    channel_ids = jnp.arange(channels, dtype=jnp.int32)
    all_hot = (channel_ids[:, None] == state_channel[0][None, :]).astype(F32)
    weighted = (ghost_amplitude[0][:, None, :] * all_hot[None]).reshape(2 * channels, states)
    ghost_matrix = jnp.concatenate(pieces(weighted, 2), axis=0)
    own_channel = lax.dynamic_slice_in_dim(state_channel[0], row_index * rows, rows, 0)
    own_surface = lax.dynamic_slice_in_dim(surface_amplitude[0], row_index * rows, rows, 0)
    depth = 128 * ((3 * channels + 127) // 128)
    slot = jnp.arange(depth, dtype=jnp.int32)
    own_hot = (
        (own_channel[:, None] == (slot % channels)[None, :]) & (slot < 3 * channels)[None, :]
    ).astype(BF16)
    half_surface = 0.5 * own_surface[:, None]

    outer0 = jnp.transpose(outer_state[0], (2, 0, 1))
    forward = [(i, i + 1) for i in range(row_count - 1)]
    backward = [(i + 1, i) for i in range(row_count - 1)]
    low = lax.ppermute(outer0[radial_here - margin :], "row", forward)
    high = lax.ppermute(outer0[:margin], "row", backward)
    near = from_first_row(outer0[: 2 * margin])

    def potential_at(points):
        radius = radius_start + spacing * points.astype(F32)
        return (threshold[0][None, :] - charge / radius[:, None])[:, :, None]

    near_potential = jnp.broadcast_to(
        potential_at(jnp.arange(2 * margin, dtype=jnp.int32)), near.shape
    )
    near_total = near[:margin]

    rounded = inner_state[0].astype(BF16)
    inner_total = inner_state[0]
    for order in range(1, TERMS + 1):
        factor = time_step / order
        sign = (factor * half_sign)[None]
        above = to_block_below(rounded)
        around = []
        for k in range(1, chips):
            around.append(chip_swap(rounded, k))
        rounded_other = core_swap(rounded)
        given, turned = lift_give(give_index, dipole_rows, rounded)
        carried = core_swap(given)
        lifted, token = lift_keep(keep_index, dipole_rows, turned, carried)
        landed = [lifted[0]]
        for k in reversed(range(1, chips)):
            landed.append(chip_swap(lifted[k], k))
        above_next = to_block_below(around[0])
        next_other = core_swap(around[0])
        own = stack(around[1:], token)
        above_own = to_block_below(own)
        own_other = core_swap(own)
        part, ghost = own_product(
            gather_index, hamiltonian_rows, ghost_matrix,
            [rounded, around[0], own, rounded_other, next_other, own_other],
        )
        slope, near, near_total = near_step(
            ghost, near, near_total, near_potential, sign, depth
        )
        vectors = jnp.stack([upper_factor, lower_factor, factor * half_sign])
        above_other = core_swap(above)
        next_above_other = core_swap(above_next)
        above_own_other = core_swap(above_own)
        settled = settle(landed)
        lower = to_block_above(settled)
        image = upper_product(
            gather_index, dipole_rows, part, own_hot, slope, half_surface, vectors,
            [above, above_next, above_own, above_other, next_above_other,
             above_own_other],
        )
        closed = close_order(image, lower, vectors, inner_total, order == TERMS)
        inner_total = closed[0]
        rounded = closed[-1]

    points = row_index * radial_here - margin + jnp.arange(
        radial_here + 2 * margin, dtype=jnp.int32
    )
    inside = (points < row_count * radial_here)[:, None, None]
    slab_potential = potential_at(points)
    w = jnp.concatenate([low, outer0, high], axis=0)
    outer_total = outer0
    for order in range(1, TERMS + 1):
        trim = slice(2 * order, points.shape[0] - 2 * order)
        w = rotate(outer_step(w, slab_potential[trim]), time_step / order)
        w = jnp.where(inside[trim], w, 0.0)
        extra = margin - 2 * order
        outer_total = outer_total + w[extra : extra + radial_here]
    first = jnp.where(row_index == 0, near_total, outer_total[:margin])
    outer_total = jnp.concatenate([first, outer_total[margin:]], axis=0)
    outer_total = jnp.transpose(outer_total, (1, 2, 0))
    return inner_total[None], outer_total[None]


def solution(mesh):
    return jax.shard_map(
        per_device,
        mesh=mesh,
        in_specs=(
            P("sym", "row", None),
            P("sym", None, None, "row"),
            P("sym", "row", None),
            P("sym", "row", None),
            P(),
            P(),
            P("sym", None, None),
            P("sym", None),
            P("sym", None),
            P("sym", None),
        ),
        out_specs=(P("sym", "row", None), P("sym", None, None, "row")),
        check_vma=False,
    )
```
